32 devices in a mesh: sta: 8 (over z, core), cell: 4 (over y, x).
Axes of the slice: x: 2, y: 2, z: 4, core: 2. Of those that a mesh axis runs over, the one named last changes fastest.
Arguments:
- station_xyz: float32 [3, 2048], P(None, 'sta'), may hold values from 0 to 1, as said below
- cell_xyz: float32 [3, 131072], P(None, 'cell'), may hold values from -0.6 to 1, as said below
- cell_weight: float32 [131072], P('cell'), may hold values from 0.3 to 3
- data: float32 [2048], P(('sta', 'cell')), may hold values from -6 to 6
- model_start: float32 [131072], P(('cell', 'sta')), may hold values from -6 to 6
Outputs:
- model_next: float32 [131072], P(('cell', 'sta'))
- residual_next: float32 [2048], P(('sta', 'cell'))
- search_next: float32 [131072], P(('cell', 'sta'))
The draws below stay inside these ranges and needn't reach their ends.
Inputs may be any that keep to these rules, and one draw needn't show every extreme that they name: `station_xyz`: rows 0 and 1 lie in [0, 1), row 2 in [0, 0.05]. `cell_xyz`: rows 0 and 1 lie in [0, 1), row 2 in [-0.6, -0.02].
All inputs are finite; a program needn't handle non-finite values.
Results may differ from the reference program's by a relative error of at most 0.0003.
Values sent between devices are 32-bit elements; how exact they have to be, the bound alone decides.
A program may use at most 64 MiB of HBM per device.

```python
import math
import jax
import jax.numpy as jnp
from jax import lax

STATIONS = 2048
CELLS = 131072


def draw_station_xyz(key, part):
    plane = jax.random.uniform(jax.random.fold_in(key, 11), (2, STATIONS), jnp.float32, 0.0, 1.0)
    height = jax.random.uniform(jax.random.fold_in(key, 12), (1, STATIONS), jnp.float32, 0.0, 0.05)
    return jnp.concatenate([plane, height], axis=0)


def draw_cell_xyz(key, part):
    plane = jax.random.uniform(jax.random.fold_in(key, 21), (2, CELLS), jnp.float32, 0.0, 1.0)
    depth = jax.random.uniform(jax.random.fold_in(key, 22), (1, CELLS), jnp.float32, -0.6, -0.02)
    return jnp.concatenate([plane, depth], axis=0)


def steps_of(rng, dims, pieces, least, high):
    gain = 1.0
    for axis_at, parts in pieces:
        steps = jax.random.uniform(jax.random.fold_in(jax.random.fold_in(rng, 6), axis_at), (parts,), jnp.float32, least / len(pieces), high / len(pieces))
        gain = gain * jnp.repeat(jnp.exp(steps), dims[axis_at] // parts).reshape((-1,) + (1,) * (len(dims) - 1 - axis_at))
    return gain


def noise(own_key, shape, spread, most, cuts=(), kind=jnp.bfloat16):
    entries = spread * jax.random.normal(own_key, shape, jnp.float32)
    if cuts:
        entries = entries * steps_of(own_key, shape, cuts, -0.22, 0.18)
    return jnp.clip(entries, -most, most).astype(kind)


def setup_inputs(seed: int = 0) -> dict:
    arg_keys = jax.random.split(jax.random.key(seed), 6)
    return {
        "station_xyz": draw_station_xyz(jax.random.fold_in(arg_keys[5], 71), 0),
        "cell_xyz": draw_cell_xyz(jax.random.fold_in(arg_keys[5], 71), 0),
        "cell_weight": jnp.clip(jnp.exp(math.log(3.0) - 2.3025851 * jax.random.uniform(arg_keys[2], (CELLS,), jnp.float32) ** steps_of(arg_keys[2], (CELLS,), ((0, 4),), -0.2, 0.2)), 0.3, 3.0),
        "data": noise(arg_keys[3], (STATIONS,), 1.0, 6.0, ((0, 32),), jnp.float32),
        "model_start": noise(arg_keys[4], (CELLS,), 1.0, 6.0, ((0, 32),), jnp.float32),
    }


SOFT = 0.0001

def kernel(sta, cel, wgt, scale):
    dx = sta[0][:, None] - cel[0][None, :]
    dy = sta[1][:, None] - cel[1][None, :]
    dz = sta[2][:, None] - cel[2][None, :]
    inv = lax.rsqrt(dx * dx + dy * dy + dz * dz + SOFT)
    return scale * dz * inv * inv * inv * wgt[None, :]

def blocked(cel, wgt):
    width = min(8192, cel.shape[1])
    count = cel.shape[1] // width
    return (jnp.transpose(cel.reshape(3, count, width), (1, 0, 2)), wgt.reshape(count, width), count, width)

def forward(sta, cel, wgt, vec, scale):
    cel_b, wgt_b, count, width = blocked(cel, wgt)
    vec_b = vec.reshape(count, width)

    def step(total, item):
        tile = kernel(sta, item[0], item[1], scale)
        return (total + jnp.dot(tile, item[2], precision=lax.Precision.HIGHEST), None)
    total, _ = lax.scan(step, jnp.zeros((sta.shape[1],), jnp.float32), (cel_b, wgt_b, vec_b))
    return total

def backward(sta, cel, wgt, res, scale):
    cel_b, wgt_b, count, width = blocked(cel, wgt)

    def one(item):
        tile = kernel(sta, item[0], item[1], scale)
        return jnp.dot(res, tile, precision=lax.Precision.HIGHEST)
    return lax.map(one, (cel_b, wgt_b)).reshape(-1)

def reference(station_xyz, cell_xyz, cell_weight, data, model_start):
    scale = 1.0 / math.sqrt(STATIONS * CELLS)
    residual = data - forward(station_xyz, cell_xyz, cell_weight, model_start, scale)
    gradient = backward(station_xyz, cell_xyz, cell_weight, residual, scale)
    gamma = jnp.sum(gradient * gradient)
    image = forward(station_xyz, cell_xyz, cell_weight, gradient, scale)
    delta = jnp.sum(image * image)
    alpha = gamma / delta
    model_next = model_start + alpha * gradient
    residual_next = residual - alpha * image
    gradient_next = backward(station_xyz, cell_xyz, cell_weight, residual_next, scale)
    gamma_next = jnp.sum(gradient_next * gradient_next)
    search_next = gradient_next + gamma_next / gamma * gradient
    return (model_next, residual_next, search_next)
```

```python
import functools
import math

import jax
import jax.numpy as jnp
from jax import lax
from jax.experimental import pallas as pl
from jax.experimental.pallas import tpu as pltpu
from jax.sharding import PartitionSpec as P

SOFT = 0.0001
LANES = 128
FEATURES = 96
MESH = pl.DeviceIdType.MESH
F32 = jnp.float32


def bf_pieces(x):
    a = x.astype(jnp.bfloat16).astype(F32)
    b = (x - a).astype(jnp.bfloat16).astype(F32)
    c = (x - a - b).astype(jnp.bfloat16).astype(F32)
    return a, b, c


def coordinate_pieces(x):
    row = lax.broadcasted_iota(jnp.int32, x.shape, 0)
    shift = jnp.where(row < 2, -0.5, jnp.where(row == 2, 0.275, 0.0))
    x = jnp.where(row < 3, x + shift, 0.0)
    h = jnp.round(x * 256.0) * (1.0 / 256.0)
    rest = x - h
    m = jnp.round(rest * 65536.0) * (1.0 / 65536.0)
    l = (rest - m).astype(jnp.bfloat16).astype(F32)
    return row, h, m, l


def norm_pieces(h, m, l, soft):
    a = jnp.sum(h * h, axis=0, keepdims=True)
    ml = m + l
    b = jnp.sum(2.0 * h * ml + ml * ml, axis=0, keepdims=True) + soft
    a1 = jnp.round(a * 256.0) * (1.0 / 256.0)
    return (a1, a - a1) + bf_pieces(b)


def rows_of(row, items):
    out = jnp.zeros(row.shape, F32)
    for at, item in items.items():
        out = jnp.where(row == at, item, out)
    return out


def cell_features(x, u, w):
    row, h, m, l = coordinate_pieces(x)
    a1, a2, b1, b2, b3 = norm_pieces(h, m, l, 0.0)
    first = h + rows_of(row, {3: 1.0, 4: 1.0, 5: a1, 6: a2})
    norms = rows_of(row, {0: 1.0, 1: 1.0, 2: 1.0, 3: b1, 4: b2, 5: b3})
    u1, u2, u3 = bf_pieces(u)
    w1, w2, w3 = bf_pieces(w)
    vectors = rows_of(row, {0: u1, 1: u2, 2: u3, 3: w1, 4: w2, 5: w3})
    zero = jnp.zeros_like(x)
    return jnp.concatenate([first, h, h, m, m, m, l, l, l, norms, vectors, zero], axis=0)


def station_features(x):
    row, h, m, l = coordinate_pieces(x)
    a1, a2, b1, b2, b3 = norm_pieces(h, m, l, SOFT)
    first = -2.0 * h + rows_of(row, {3: a1, 4: a2, 5: 1.0, 6: 1.0})
    norms = rows_of(row, {0: b1, 1: b2, 2: b3, 3: 1.0, 4: 1.0, 5: 1.0})
    h, m, l = -2.0 * h, -2.0 * m, -2.0 * l
    zero = jnp.zeros_like(x)
    return jnp.concatenate([first, m, l, h, m, l, h, m, l, norms, zero, zero], axis=0)


def spread_matrix():
    row = lax.broadcasted_iota(jnp.int32, (FEATURES, 3 * LANES), 0)
    col = lax.broadcasted_iota(jnp.int32, (FEATURES, 3 * LANES), 1)
    z = (row == 2) | (row == 26) | (row == 50)
    u = (row >= 80) & (row < 83)
    w = (row >= 83) & (row < 86)
    pick = ((col < LANES) & z) | ((col >= LANES) & (col < 2 * LANES) & u) | ((col >= 2 * LANES) & w)
    return jnp.where(pick, 1.0, 0.0).astype(jnp.bfloat16)


def kernel(sizes, st_ref, cell_ref, w_ref, m_ref, data_ref, model_ref, res_ref, search_ref,
           kmat, lhs, czb, ub, wb, gb, grow, st_all, szb, rbc, rs1, rs2, ag1, ag2, gn, out1, out2,
           send_sem, recv_sem):
    n_sta, n_cell, cells, width, piece, scale, mb = sizes
    n = n_sta * n_cell
    groups = cells // 8
    blocks = cells // LANES
    per_tile = LANES // piece
    tiles = width // LANES
    my_sta, my_cell = lax.axis_index("sta"), lax.axis_index("cell")
    me = my_sta * n_cell + my_cell

    def peer(k):
        flat = lax.rem(me + k, n)
        return (flat // n_cell, lax.rem(flat, n_cell))

    barrier = pltpu.get_barrier_semaphore()

    def greet(k, c):
        pl.semaphore_signal(barrier, inc=1, device_id=peer(k), device_id_type=MESH)
        return c

    lax.fori_loop(1, n, greet, 0)

    lane = lax.broadcasted_iota(jnp.int32, (1, LANES), 1)
    own = lane < piece

    spread = spread_matrix()

    def prepare(b, c):
        at = pl.multiple_of(b * LANES, LANES)
        cols = pl.ds(at, LANES)
        w = w_ref[:, cols] * scale
        feats = cell_features(cell_ref[:, cols], w * m_ref[:, cols], w)
        rows = jnp.transpose(feats).astype(jnp.bfloat16)
        lhs[cols, :] = rows
        wide = jnp.dot(rows, spread, preferred_element_type=F32)
        gs = pl.ds(b * (LANES // 8), LANES // 8)
        czb[gs] = wide[:, :LANES].reshape(LANES // 8, 8, LANES) - 0.275
        ub[gs] = wide[:, LANES:2 * LANES].reshape(LANES // 8, 8, LANES)
        wb[gs] = wide[:, 2 * LANES:].reshape(LANES // 8, 8, LANES)
        return c

    lax.fori_loop(0, blocks, prepare, 0)

    st_all[my_sta] = st_ref[...]
    pl.semaphore_wait(barrier, n - 1)

    def send_stations(k, c):
        pltpu.make_async_remote_copy(
            src_ref=st_ref, dst_ref=st_all.at[my_sta], send_sem=send_sem.at[0], recv_sem=recv_sem.at[0],
            device_id=(lax.rem(my_sta + k, n_sta), my_cell), device_id_type=MESH).start()
        return c

    lax.fori_loop(1, n_sta, send_stations, 0)

    def bulk_wait(buf, count, sems, which):
        part = buf.at[pl.ds(0, count)]
        pltpu.make_async_copy(part, part, sems.at[which]).wait()

    def send_block(out, rs, which, k, s, rows, fill):
        for c in range(n_cell):
            tile, q = (c * piece) // LANES, c % per_tile
            value = rows[tile]
            if q:
                value = pltpu.roll(value, LANES - q * piece, 1)
            if fill is not None:
                value = jnp.where(own, value, fill)
            out[s * n_cell + c] = value
        for c in range(n_cell):
            target = s * n_cell + c

            @pl.when(target != me)
            def _():
                pltpu.make_async_remote_copy(
                    src_ref=out.at[target], dst_ref=rs.at[me], send_sem=send_sem.at[which],
                    recv_sem=recv_sem.at[which], device_id=(s, c), device_id_type=MESH).start()

            @pl.when(target == me)
            def _():
                rs[me] = out[target]

    def broadcast(buf, which):
        def one(k, c):
            pltpu.make_async_remote_copy(
                src_ref=buf.at[me], dst_ref=buf.at[me], send_sem=send_sem.at[which],
                recv_sem=recv_sem.at[which], device_id=peer(k), device_id_type=MESH).start()
            return c
        lax.fori_loop(1, n, one, 0)

    def total(buf):
        return jnp.sum(buf[...], axis=0)

    def sta_block(k, c):
        s = lax.rem(my_sta + k, n_sta)

        @pl.when(k == 1)
        def _():
            bulk_wait(st_all, n_sta - 1, recv_sem, 0)

        x = st_all[s]
        rhs = station_features(x).astype(jnp.bfloat16)
        sz = jnp.broadcast_to(x[2:3, :], (8, width))

        def block(b, accs):
            at = pl.multiple_of(b * mb, mb)
            r2 = jnp.dot(lhs[pl.ds(at, mb), :], rhs, preferred_element_type=F32)
            gs = pl.ds(b * (mb // 8), mb // 8)
            cz, u = czb[gs], ub[gs]
            out = []
            for t in range(tiles):
                part = r2[:, t * LANES:(t + 1) * LANES].reshape(mb // 8, 8, LANES)
                inv = lax.rsqrt(part)
                dz = sz[None, :, t * LANES:(t + 1) * LANES] - cz
                value = (dz * inv) * (inv * inv)
                kmat[s, gs, :, t * LANES:(t + 1) * LANES] = value
                out.append(accs[t] + jnp.sum(value * u, axis=0))
            return tuple(out)

        accs = lax.fori_loop(0, cells // mb, block, tuple(jnp.zeros((8, LANES), F32) for _ in range(tiles)))
        rows = [jnp.sum(a, axis=0, keepdims=True) for a in accs]
        send_block(out1, rs1, 1, k, s, rows, None)
        return c

    lax.fori_loop(0, n_sta, sta_block, 0)
    bulk_wait(rs1, n - 1, recv_sem, 1)
    ag1[me] = data_ref[...] - total(rs1)
    broadcast(ag1, 2)

    def spread_rows(buf, dst):
        def one(s, c):
            for t in range(tiles):
                row = jnp.zeros((1, LANES), F32)
                for q in range(per_tile):
                    value = jnp.where(own, buf[s * n_cell + t * per_tile + q], 0.0)
                    if q:
                        value = pltpu.roll(value, q * piece, 1)
                    row = row + value
                dst[s, :, t * LANES:(t + 1) * LANES] = jnp.broadcast_to(row, (8, LANES))
            return c
        lax.fori_loop(0, n_sta, one, 0)

    bulk_wait(ag1, n - 1, recv_sem, 2)
    spread_rows(ag1, rbc)

    step = 8

    def backward(b, sq):
        gs = pl.ds(b * step, step)
        acc = jnp.zeros((step, 8, LANES), F32)
        for s in range(n_sta):
            for t in range(tiles):
                cols = slice(t * LANES, (t + 1) * LANES)
                acc = acc + kmat[s, gs, :, cols] * rbc[s, :, cols][None]
        g = jnp.sum(acc, axis=2, keepdims=True) * wb[gs]
        gb[gs] = g
        return sq + jnp.sum(g * g, axis=0)

    sq = lax.fori_loop(0, groups // step, backward, jnp.zeros((8, LANES), F32))
    gamma_part = jnp.sum(sq, axis=0, keepdims=True)

    def weigh(b, c):
        gs = pl.ds(b * 16, 16)
        ub[gs] = gb[gs] * wb[gs]
        return c

    lax.fori_loop(0, groups // 16, weigh, 0)

    together = 4

    def image_block(k, c):
        ss = [lax.rem(my_sta + k * together + i, n_sta) for i in range(together)]

        def block(b, accs):
            gs = pl.ds(b * 8, 8)
            u = ub[gs]
            out = []
            for i in range(together):
                for t in range(tiles):
                    value = kmat[ss[i], gs, :, t * LANES:(t + 1) * LANES] * u
                    out.append(accs[i * tiles + t] + jnp.sum(value, axis=0))
            return tuple(out)

        accs = lax.fori_loop(0, groups // 8, block,
                             tuple(jnp.zeros((8, LANES), F32) for _ in range(together * tiles)))
        for i in range(together):
            rows = [jnp.sum(a, axis=0, keepdims=True) for a in accs[i * tiles:(i + 1) * tiles]]
            send_block(out2, rs2, 3, k, ss[i], rows, gamma_part)
        return c

    lax.fori_loop(0, n_sta // together, image_block, 0)
    eye = (lax.broadcasted_iota(jnp.int32, (16, 8, LANES), 0) * 8
           + lax.broadcasted_iota(jnp.int32, (16, 8, LANES), 1)
           == lax.broadcasted_iota(jnp.int32, (16, 8, LANES), 2))

    def as_row(b):
        block = jnp.where(eye, gb[pl.ds(b * 16, 16)], 0.0)
        return jnp.sum(jnp.sum(block, axis=0), axis=0, keepdims=True)

    bulk_wait(rs2, n - 1, recv_sem, 3)
    ag2[me] = total(rs2)
    broadcast(ag2, 4)

    def keep_row(b, c):
        grow[:, pl.ds(pl.multiple_of(b * LANES, LANES), LANES)] = as_row(b)
        return c

    lax.fori_loop(0, blocks, keep_row, 0)
    bulk_wait(ag2, n - 1, recv_sem, 4)
    images = jnp.where(own[None], ag2[...], 0.0)
    delta = jnp.sum(jnp.sum(images * images, axis=0), axis=1, keepdims=True)
    mine = ag2[me]
    gamma = jnp.sum(jnp.where(lane == piece, mine, 0.0), axis=1, keepdims=True)
    alpha = gamma / delta
    res_ref[...] = ag1[me] - alpha * mine
    ag1_next = ag1[...] - alpha[None] * ag2[...]
    rs1[...] = ag1_next
    spread_rows(rs1, rbc)

    sq = lax.fori_loop(0, groups // step, backward, jnp.zeros((8, LANES), F32))
    gn[me] = jnp.sum(sq, axis=0, keepdims=True)
    broadcast(gn, 5)

    def next_row(b, c):
        cols = pl.ds(pl.multiple_of(b * LANES, LANES), LANES)
        search_ref[:, cols] = as_row(b)
        model_ref[:, cols] = m_ref[:, cols] + alpha * grow[:, cols]
        return c

    lax.fori_loop(0, blocks, next_row, 0)
    bulk_wait(gn, n - 1, recv_sem, 5)
    beta = total(gn)[:, :1] / gamma
    search_ref[...] = search_ref[...] + beta * grow[...]

    bulk_wait(st_all, n_sta - 1, send_sem, 0)
    for which, buf in ((1, rs1), (2, ag1), (3, rs2), (4, ag2), (5, gn)):
        bulk_wait(buf, n - 1, send_sem, which)


def per_device(station_xyz, cell_xyz, cell_weight, data, model_start):
    n_sta, n_cell = lax.axis_size("sta"), lax.axis_size("cell")
    n = n_sta * n_cell
    width = station_xyz.shape[1]
    cells = model_start.shape[0]
    piece = data.shape[0]
    scale = 1.0 / math.sqrt(width * n_sta * cells * n)
    at = lax.axis_index("sta") * cells
    own_cells = jnp.pad(lax.dynamic_slice_in_dim(cell_xyz, at, cells, 1), ((0, 5), (0, 0)))
    own_weight = lax.dynamic_slice_in_dim(cell_weight, at, cells, 0).reshape(1, cells)
    stations = jnp.pad(station_xyz, ((0, 5), (0, 0)))
    data_row = jnp.pad(data, (0, LANES - piece)).reshape(1, LANES)
    groups = cells // 8
    mb = min(1024, cells)
    sizes = (n_sta, n_cell, cells, width, piece, scale, mb)
    vmem = pl.BlockSpec(memory_space=pltpu.VMEM)
    wide = pltpu.VMEM((groups, 8, LANES), F32)
    message = pltpu.VMEM((n, 1, LANES), F32)
    model_next, residual, search = pl.pallas_call(
        functools.partial(kernel, sizes),
        out_shape=(jax.ShapeDtypeStruct((1, cells), F32), jax.ShapeDtypeStruct((1, LANES), F32),
                   jax.ShapeDtypeStruct((1, cells), F32)),
        in_specs=[vmem] * 5,
        out_specs=(vmem, vmem, vmem),
        scratch_shapes=[
            pltpu.VMEM((n_sta, groups, 8, width), F32),
            pltpu.VMEM((cells, FEATURES), jnp.bfloat16),
            wide, wide, wide, wide,
            pltpu.VMEM((1, cells), F32),
            pltpu.VMEM((n_sta, 8, width), F32),
            pltpu.VMEM((n_sta, 8, width), F32),
            pltpu.VMEM((n_sta, 8, width), F32),
            message, message, message, message, message, message, message,
            pltpu.SemaphoreType.DMA((6,)),
            pltpu.SemaphoreType.DMA((6,)),
        ],
        compiler_params=pltpu.CompilerParams(
            collective_id=0, has_side_effects=True, vmem_limit_bytes=60 * 1024 * 1024),
    )(stations, own_cells, own_weight, model_start.reshape(1, cells), data_row)
    return (model_next.reshape(cells), residual[0, :piece], search.reshape(cells))


def solution(mesh):
    placed = (P(None, "sta"), P(None, "cell"), P("cell"), P(("sta", "cell")), P(("cell", "sta")))
    return jax.shard_map(
        per_device,
        mesh=mesh,
        in_specs=placed,
        out_specs=(P(("cell", "sta")), P(("sta", "cell")), P(("cell", "sta"))),
        check_vma=False,
    )
```

```python
import functools
import math

import jax
import jax.numpy as jnp
from jax import lax
from jax.experimental import pallas as pl
from jax.experimental.pallas import tpu as pltpu
from jax.sharding import PartitionSpec as P

SOFT = 0.0001
LANES = 128
FEATURES = 96
MESH = pl.DeviceIdType.MESH
F32 = jnp.float32


def bf_pieces(x):
    a = x.astype(jnp.bfloat16).astype(F32)
    b = (x - a).astype(jnp.bfloat16).astype(F32)
    c = (x - a - b).astype(jnp.bfloat16).astype(F32)
    return a, b, c


def coordinate_pieces(x):
    row = lax.broadcasted_iota(jnp.int32, x.shape, 0)
    shift = jnp.where(row < 2, -0.5, jnp.where(row == 2, 0.275, 0.0))
    x = jnp.where(row < 3, x + shift, 0.0)
    h = jnp.round(x * 256.0) * (1.0 / 256.0)
    rest = x - h
    m = jnp.round(rest * 65536.0) * (1.0 / 65536.0)
    l = (rest - m).astype(jnp.bfloat16).astype(F32)
    return row, h, m, l


def norm_pieces(h, m, l, soft):
    a = jnp.sum(h * h, axis=0, keepdims=True)
    ml = m + l
    b = jnp.sum(2.0 * h * ml + ml * ml, axis=0, keepdims=True) + soft
    a1 = jnp.round(a * 256.0) * (1.0 / 256.0)
    return (a1, a - a1) + bf_pieces(b)


def rows_of(row, items):
    out = jnp.zeros(row.shape, F32)
    for at, item in items.items():
        out = jnp.where(row == at, item, out)
    return out


def cell_features(x, u, w):
    row, h, m, l = coordinate_pieces(x)
    a1, a2, b1, b2, b3 = norm_pieces(h, m, l, 0.0)
    first = h + rows_of(row, {3: 1.0, 4: 1.0, 5: a1, 6: a2})
    norms = rows_of(row, {0: 1.0, 1: 1.0, 2: 1.0, 3: b1, 4: b2, 5: b3})
    u1, u2, u3 = bf_pieces(u)
    w1, w2, w3 = bf_pieces(w)
    vectors = rows_of(row, {0: u1, 1: u2, 2: u3, 3: w1, 4: w2, 5: w3})
    zero = jnp.zeros_like(x)
    return jnp.concatenate([first, h, h, m, m, m, l, l, l, norms, vectors, zero], axis=0)


def station_features(x):
    row, h, m, l = coordinate_pieces(x)
    a1, a2, b1, b2, b3 = norm_pieces(h, m, l, SOFT)
    first = -2.0 * h + rows_of(row, {3: a1, 4: a2, 5: 1.0, 6: 1.0})
    norms = rows_of(row, {0: b1, 1: b2, 2: b3, 3: 1.0, 4: 1.0, 5: 1.0})
    h, m, l = -2.0 * h, -2.0 * m, -2.0 * l
    zero = jnp.zeros_like(x)
    return jnp.concatenate([first, m, l, h, m, l, h, m, l, norms, zero, zero], axis=0)


def spread_matrix():
    row = lax.broadcasted_iota(jnp.int32, (FEATURES, 3 * LANES), 0)
    col = lax.broadcasted_iota(jnp.int32, (FEATURES, 3 * LANES), 1)
    z = (row == 2) | (row == 26) | (row == 50)
    u = (row >= 80) & (row < 83)
    w = (row >= 83) & (row < 86)
    pick = ((col < LANES) & z) | ((col >= LANES) & (col < 2 * LANES) & u) | ((col >= 2 * LANES) & w)
    return jnp.where(pick, 1.0, 0.0).astype(jnp.bfloat16)


def kernel(sizes, st_ref, cell_ref, w_ref, m_ref, data_ref, model_ref, res_ref, search_ref,
           kmat, lhs, czb, ub, wb, gb, grow, st_all, szb, rbc, rs1, rs2, ag1, ag2, gm, gn, out1, out2,
           send_sem, recv_sem):
    n_sta, n_cell, cells, width, piece, scale, mb = sizes
    n = n_sta * n_cell
    groups = cells // 8
    blocks = cells // LANES
    per_tile = LANES // piece
    tiles = width // LANES
    my_sta, my_cell = lax.axis_index("sta"), lax.axis_index("cell")
    me = my_sta * n_cell + my_cell

    def peer(k):
        flat = lax.rem(me + k, n)
        return (flat // n_cell, lax.rem(flat, n_cell))

    barrier = pltpu.get_barrier_semaphore()

    def greet(k, c):
        pl.semaphore_signal(barrier, inc=1, device_id=peer(k), device_id_type=MESH)
        return c

    lax.fori_loop(1, n, greet, 0)

    lane = lax.broadcasted_iota(jnp.int32, (1, LANES), 1)
    own = lane < piece

    spread = spread_matrix()

    def prepare(b, c):
        at = pl.multiple_of(b * LANES, LANES)
        cols = pl.ds(at, LANES)
        w = w_ref[:, cols] * scale
        feats = cell_features(cell_ref[:, cols], w * m_ref[:, cols], w)
        rows = jnp.transpose(feats).astype(jnp.bfloat16)
        lhs[cols, :] = rows
        wide = jnp.dot(rows, spread, preferred_element_type=F32)
        gs = pl.ds(b * (LANES // 8), LANES // 8)
        czb[gs] = wide[:, :LANES].reshape(LANES // 8, 8, LANES) - 0.275
        ub[gs] = wide[:, LANES:2 * LANES].reshape(LANES // 8, 8, LANES)
        wb[gs] = wide[:, 2 * LANES:].reshape(LANES // 8, 8, LANES)
        return c

    lax.fori_loop(0, blocks, prepare, 0, unroll=4)

    st_all[my_sta] = st_ref[...]
    pl.semaphore_wait(barrier, n - 1)

    def send_stations(k, c):
        pltpu.make_async_remote_copy(
            src_ref=st_ref, dst_ref=st_all.at[my_sta], send_sem=send_sem.at[0], recv_sem=recv_sem.at[0],
            device_id=(lax.rem(my_sta + k, n_sta), my_cell), device_id_type=MESH).start()
        return c

    lax.fori_loop(1, n_sta, send_stations, 0)

    def bulk_wait(buf, count, sems, which):
        part = buf.at[pl.ds(0, count)]
        pltpu.make_async_copy(part, part, sems.at[which]).wait()

    def send_block(out, rs, which, s, rows):
        row = jnp.concatenate(rows, axis=1)
        out[s] = row
        rs[me, s] = row

        def one(k, c):
            pltpu.make_async_remote_copy(
                src_ref=out.at[s], dst_ref=rs.at[me, s], send_sem=send_sem.at[which],
                recv_sem=recv_sem.at[which], device_id=peer(k), device_id_type=MESH).start()
            return c

        lax.fori_loop(1, n, one, 0)

    def own_piece(row):
        out = jnp.zeros((1, LANES), F32)
        for c in range(n_cell):
            tile, q = (c * piece) // LANES, c % per_tile
            value = row[:, tile * LANES:(tile + 1) * LANES]
            if q:
                value = pltpu.roll(value, LANES - q * piece, 1)
            out = jnp.where(my_cell == c, value, out)
        return out

    def broadcast(buf, which):
        def one(k, c):
            pltpu.make_async_remote_copy(
                src_ref=buf.at[me], dst_ref=buf.at[me], send_sem=send_sem.at[which],
                recv_sem=recv_sem.at[which], device_id=peer(k), device_id_type=MESH).start()
            return c
        lax.fori_loop(1, n, one, 0)

    def total(buf):
        return jnp.sum(buf[...], axis=0)

    def sta_block(k, c):
        s = lax.rem(my_sta + k, n_sta)

        @pl.when(k == 1)
        def _():
            bulk_wait(st_all, n_sta - 1, recv_sem, 0)

        x = st_all[s]
        rhs = station_features(x).astype(jnp.bfloat16)
        sz = jnp.broadcast_to(x[2:3, :], (8, width))

        def block(b, accs):
            at = pl.multiple_of(b * mb, mb)
            r2 = jnp.dot(lhs[pl.ds(at, mb), :], rhs, preferred_element_type=F32)
            gs = pl.ds(b * (mb // 8), mb // 8)
            cz, u = czb[gs], ub[gs]
            out = []
            for t in range(tiles):
                part = r2[:, t * LANES:(t + 1) * LANES].reshape(mb // 8, 8, LANES)
                inv = lax.rsqrt(part)
                dz = sz[None, :, t * LANES:(t + 1) * LANES] - cz
                value = (dz * inv) * (inv * inv)
                kmat[s, gs, :, t * LANES:(t + 1) * LANES] = value
                out.append(accs[t] + jnp.sum(value * u, axis=0))
            return tuple(out)

        accs = lax.fori_loop(0, cells // mb, block, tuple(jnp.zeros((8, LANES), F32) for _ in range(tiles)))
        rows = [jnp.sum(a, axis=0, keepdims=True) for a in accs]
        first = jnp.where(k == 0, 1.0, 0.0)
        for q in range(n_cell):
            tile, at = (q * piece) // LANES, q % per_tile
            value = jnp.where(own, data_ref[...], 0.0) * jnp.where(my_cell == q, first, 0.0)
            if at:
                value = pltpu.roll(value, at * piece, 1)
            rows[tile] = rows[tile] - value
        send_block(out1, rs1, 1, s, rows)
        return c

    lax.fori_loop(0, n_sta, sta_block, 0)
    bulk_wait(rs1, n - 1, recv_sem, 1)

    def residual(s, c):
        row = -jnp.sum(rs1[:, s], axis=0)
        ag1[s] = row
        rbc[s] = jnp.broadcast_to(row, (8, width))
        return c

    lax.fori_loop(0, n_sta, residual, 0)

    step = 8

    def backward(b, c):
        gs = pl.ds(b * step, step)
        acc = jnp.zeros((step, 8, LANES), F32)
        for s in range(n_sta):
            for t in range(tiles):
                cols = slice(t * LANES, (t + 1) * LANES)
                acc = acc + kmat[s, gs, :, cols] * rbc[s, :, cols][None]
        gb[gs] = acc
        return c

    ones = jnp.ones((3 * LANES, LANES), jnp.bfloat16)
    eye = (lax.broadcasted_iota(jnp.int32, (16, 8, LANES), 0) * 8
           + lax.broadcasted_iota(jnp.int32, (16, 8, LANES), 1)
           == lax.broadcasted_iota(jnp.int32, (16, 8, LANES), 2))

    def finish(dst, b, sq):
        gs = pl.ds(b * 16, 16)
        parts = jnp.concatenate(bf_pieces(gb[gs].reshape(LANES, LANES)), axis=1).astype(jnp.bfloat16)
        w = wb[gs]
        g = jnp.dot(parts, ones, preferred_element_type=F32).reshape(16, 8, LANES) * w
        ub[gs] = g * w
        row = jnp.sum(jnp.sum(jnp.where(eye, g, 0.0), axis=0), axis=0, keepdims=True)
        dst[:, pl.ds(pl.multiple_of(b * LANES, LANES), LANES)] = row
        return sq + row * row

    def gradient(dst):
        lax.fori_loop(0, groups // step, backward, 0)
        sq = lax.fori_loop(0, blocks, functools.partial(finish, dst), jnp.zeros((1, LANES), F32), unroll=4)
        return jnp.broadcast_to(jnp.sum(sq, axis=1, keepdims=True), (1, LANES))

    gm[me] = gradient(grow)
    broadcast(gm, 2)

    together = 4

    def image_block(k, c):
        ss = [lax.rem(my_sta + k * together + i, n_sta) for i in range(together)]

        def block(b, accs):
            gs = pl.ds(b * 8, 8)
            u = ub[gs]
            out = []
            for i in range(together):
                for t in range(tiles):
                    value = kmat[ss[i], gs, :, t * LANES:(t + 1) * LANES] * u
                    out.append(accs[i * tiles + t] + jnp.sum(value, axis=0))
            return tuple(out)

        accs = lax.fori_loop(0, groups // 8, block,
                             tuple(jnp.zeros((8, LANES), F32) for _ in range(together * tiles)))
        for i in range(together):
            rows = [jnp.sum(a, axis=0, keepdims=True) for a in accs[i * tiles:(i + 1) * tiles]]
            send_block(out2, rs2, 3, ss[i], rows)
        return c

    lax.fori_loop(0, n_sta // together, image_block, 0)
    bulk_wait(gm, n - 1, recv_sem, 2)
    gamma = total(gm)[:, :1]
    bulk_wait(rs2, n - 1, recv_sem, 3)

    def image_sum(s, sq):
        row = jnp.sum(rs2[:, s], axis=0)
        ag2[s] = row
        return sq + row * row

    sq = lax.fori_loop(0, n_sta, image_sum, jnp.zeros((1, width), F32))
    alpha = gamma / jnp.sum(sq, axis=1, keepdims=True)

    def residual_next(s, c):
        rbc[s] = jnp.broadcast_to(ag1[s] - alpha * ag2[s], (8, width))
        return c

    lax.fori_loop(0, n_sta, residual_next, 0)
    res_ref[...] = own_piece(ag1[my_sta] - alpha * ag2[my_sta])

    gn[me] = gradient(search_ref)
    broadcast(gn, 5)
    model_ref[...] = m_ref[...] + alpha * grow[...]
    bulk_wait(gn, n - 1, recv_sem, 5)
    beta = total(gn)[:, :1] / gamma
    search_ref[...] = search_ref[...] + beta * grow[...]

    bulk_wait(st_all, n_sta - 1, send_sem, 0)
    for which, buf in ((1, rs1), (2, gm), (3, rs2), (5, gn)):
        bulk_wait(buf, n - 1, send_sem, which)


def per_device(station_xyz, cell_xyz, cell_weight, data, model_start):
    n_sta, n_cell = lax.axis_size("sta"), lax.axis_size("cell")
    n = n_sta * n_cell
    width = station_xyz.shape[1]
    cells = model_start.shape[0]
    piece = data.shape[0]
    scale = 1.0 / math.sqrt(width * n_sta * cells * n)
    at = lax.axis_index("sta") * cells
    own_cells = jnp.pad(lax.dynamic_slice_in_dim(cell_xyz, at, cells, 1), ((0, 5), (0, 0)))
    own_weight = lax.dynamic_slice_in_dim(cell_weight, at, cells, 0).reshape(1, cells)
    stations = jnp.pad(station_xyz, ((0, 5), (0, 0)))
    data_row = jnp.pad(data, (0, LANES - piece)).reshape(1, LANES)
    groups = cells // 8
    mb = min(1024, cells)
    sizes = (n_sta, n_cell, cells, width, piece, scale, mb)
    vmem = pl.BlockSpec(memory_space=pltpu.VMEM)
    wide = pltpu.VMEM((groups, 8, LANES), F32)
    whole = pltpu.VMEM((n, n_sta, 1, width), F32)
    line = pltpu.VMEM((n_sta, 1, width), F32)
    message = pltpu.VMEM((n, 1, LANES), F32)
    model_next, residual, search = pl.pallas_call(
        functools.partial(kernel, sizes),
        out_shape=(jax.ShapeDtypeStruct((1, cells), F32), jax.ShapeDtypeStruct((1, LANES), F32),
                   jax.ShapeDtypeStruct((1, cells), F32)),
        in_specs=[vmem] * 5,
        out_specs=(vmem, vmem, vmem),
        scratch_shapes=[
            pltpu.VMEM((n_sta, groups, 8, width), F32),
            pltpu.VMEM((cells, FEATURES), jnp.bfloat16),
            wide, wide, wide, wide,
            pltpu.VMEM((1, cells), F32),
            pltpu.VMEM((n_sta, 8, width), F32),
            pltpu.VMEM((n_sta, 8, width), F32),
            pltpu.VMEM((n_sta, 8, width), F32),
            whole, whole, line, line, message, message, line, line,
            pltpu.SemaphoreType.DMA((6,)),
            pltpu.SemaphoreType.DMA((6,)),
        ],
        compiler_params=pltpu.CompilerParams(
            collective_id=0, has_side_effects=True, vmem_limit_bytes=60 * 1024 * 1024),
    )(stations, own_cells, own_weight, model_start.reshape(1, cells), data_row)
    return (model_next.reshape(cells), residual[0, :piece], search.reshape(cells))


def solution(mesh):
    placed = (P(None, "sta"), P(None, "cell"), P("cell"), P(("sta", "cell")), P(("cell", "sta")))
    return jax.shard_map(
        per_device,
        mesh=mesh,
        in_specs=placed,
        out_specs=(P(("cell", "sta")), P(("sta", "cell")), P(("cell", "sta"))),
        check_vma=False,
    )
```
